256 devices in a mesh: group: 4 (over x, y), expert: 32 (over z), tensor: 2 (over core).
Axes of the slice: x: 2, y: 2, z: 32, core: 2. Of those that a mesh axis runs over, the one named last changes fastest.
The devices are a block of a 4x8x32 slice.
Arguments:
- tokens: bfloat16 [8192, 4096], P(('group', 'expert', 'tensor')), parts along dimension 0, may hold values from -600 to 600
- norm_gain: float32 [4096], replicated, may hold values from 0.1 to 1.9
- w_gate: bfloat16 [32, 4096, 768], P('expert', None, 'tensor'), may hold values from -0.09375 to 0.09375
- w_up: bfloat16 [32, 4096, 768], P('expert', None, 'tensor'), may hold values from -0.09375 to 0.09375
- w_down: bfloat16 [32, 768, 4096], P('expert', 'tensor'), may hold values from -0.4375 to 0.4375
- expert_ids: int32 [8192, 8], P(('group', 'expert', 'tensor')), parts along dimension 0, may hold values from 0 to 31, all different within a row; in each aligned block of 32 rows (0 to 31, 32 to 63, ...) at most 16 rows name the same one
- route_weights: float32 [8192, 8], P(('group', 'expert', 'tensor')), parts along dimension 0, may hold values from 0.05 to 1
Outputs:
- mixed: bfloat16 [8192, 4096], P(('group', 'expert', 'tensor')), parts along dimension 0
The draws below stay inside these ranges and needn't reach their ends.
There are 4 independent parts, one for each index of `group`. The reference program is written for one: setup_inputs(seed, part) draws one part's arguments, and reference() takes and returns one part's arrays. A program takes and returns all parts, laid end to end along the dimension named above; an argument that names none is the same for every part. Nothing has to cross between parts.
Inputs may be any that keep to these rules, and one draw needn't show every extreme that they name: `expert_ids`: each row names 8 different experts. Among the 32 rows of one device no expert is named more than 16 times, and in every draw some device names some expert exactly 16 times.
All inputs are finite; a program needn't handle non-finite values.
Results may differ from the reference program's by a relative error of at most 0.0077.
Values may be sent and summed in bfloat16 or wider, within the bound.
No kernel may reach another device: no remote copies, remote signals or barrier semaphores. Data moves between devices by JAX's collectives and lax.ppermute only.
A program may use at most 128 MiB of HBM per device.

```python
import math
import jax
import jax.numpy as jnp
import numpy as np
from jax import lax

D = 4096
EXPERT_FF = 768
TOPK = 8
TOK_DEV = 32
EXPERTS = 32
CAP = 16
TOKENS = 2048
N_EXPERT = 32
N_TENSOR = 2


def draw_tokens(key, part):
    first, second, third = jax.random.split(jax.random.fold_in(key, 7), 3)
    base = jnp.clip(jax.random.normal(first, (TOKENS, D), jnp.float32), -6.0, 6.0)
    columns = jnp.exp(jax.random.uniform(second, (1, D), jnp.float32, 0.0, math.log(10.0)))
    rowscale = jnp.exp(jax.random.uniform(third, (TOKENS, 1), jnp.float32, 0.0, math.log(10.0)))
    return (base * columns * rowscale).astype(jnp.bfloat16)


def level_of(stream_key, dims, shards, least, largest):
    def one(dim, shards_of):
        draws = jax.random.uniform(jax.random.fold_in(jax.random.fold_in(stream_key, 6), dim), (shards_of,), jnp.float32, least / len(shards), largest / len(shards))
        return jnp.repeat(jnp.exp(draws), dims[dim] // shards_of).reshape((-1,) + (1,) * (len(dims) - dim - 1))

    loudness = one(*shards[0])
    for cut in shards[1:]:
        loudness = loudness * one(*cut)
    return loudness


def deal_out(key, own, number, rows, count, top, reach, skew):
    ranking = jax.random.permutation(key, count)
    crowded, usual = portions_of(count, rows * top, reach, skew, True), portions_of(count, rows * top, reach, skew, False)
    places = jnp.arange(count)

    def named(tallies, offset_by):
        used = int((tallies > 0).sum())
        fixed = max(1, used // 4)
        passed = fixed + (places - fixed + offset_by * (used - fixed)) % max(1, count - fixed)
        return jnp.zeros((count,), jnp.int32).at[ranking[jnp.where(places < fixed, places, passed)]].set(jnp.asarray(tallies, jnp.int32))

    tallies = jnp.where(number % 4 == 0, named(crowded, number // 4), named(usual, number - number // 4 - 1))
    mixed = jax.random.permutation(jax.random.fold_in(own, 3), count)
    donor, taker = mixed[0:count // 2 * 2:2], mixed[1:count // 2 * 2:2]
    margin = jnp.minimum(tallies[donor] - 1, reach - tallies[taker]) // 2
    margin = jnp.where((donor == ranking[0]) | (taker == ranking[0]) | (tallies[taker] == 0), 0, jnp.maximum(margin, 0))
    passed = jax.random.randint(jax.random.fold_in(own, 4), (count // 2,), 0, 1 << 20) % (margin + 1)
    tallies = tallies.at[donor].add(-passed).at[taker].add(passed)
    labels = jnp.searchsorted(jnp.cumsum(tallies), jnp.arange(rows * top), side="right").astype(jnp.int32)
    table = labels.reshape(top, rows).T
    table = table[jax.random.permutation(jax.random.fold_in(own, 1), rows)]
    offset_by = jax.random.randint(jax.random.fold_in(own, 2), (rows, 1), 0, top)
    return jnp.take_along_axis(table, (jnp.arange(top)[None, :] + offset_by) % top, axis=1)


def portions_of(amount, total, bound, lean, full):
    portions = [(1 << 20) // math.isqrt(rank ** lean) + 1 for rank in range(1, amount + 1)]
    largest = bound if full else min(bound, max(-(-total // amount), total * portions[0] // sum(portions)))
    least = 1 if total - largest >= amount - 1 else 0
    holding, surplus = [largest] + [least] * (amount - 1), total - largest - least * (amount - 1)
    while surplus > 0:
        free = [i for i in range(1, amount) if holding[i] < largest] or [i for i in range(1, amount) if holding[i] < bound]
        mass, left = sum([portions[i] for i in free]), surplus
        for i in free:
            extra = min(bound - holding[i], max(1, left * portions[i] // mass), surplus)
            holding[i] = holding[i] + extra
            surplus = surplus - extra
    return np.array(holding)


def centred(key, shape, deviation, most, cuts=(), kind=jnp.bfloat16):
    loudness = level_of(key, shape, cuts, -0.22, 0.18) if cuts else 1.0
    result = jax.random.normal(key, shape, jnp.float32) * deviation * loudness
    return jnp.minimum(jnp.maximum(result, -most), most).astype(kind)


def setup_inputs(seed: int = 0, part: int = 0) -> dict:
    key_list = jax.random.split(jax.random.key(seed), 8)
    part_splits = jax.random.split(jax.random.fold_in(key_list[7], part), 8)
    tokens = draw_tokens(jax.random.fold_in(jax.random.fold_in(key_list[7], part), 71), part)
    norm_gain = jnp.clip(1.0 + 0.18 * jax.random.normal(key_list[1], (D,), jnp.float32), 0.1, 1.9)
    w_gate = centred(key_list[2], (EXPERTS, D, EXPERT_FF), D ** -0.5, 0.09375, ((0, 32), (2, 2)))
    w_up = centred(key_list[3], (EXPERTS, D, EXPERT_FF), D ** -0.5, 0.09375, ((0, 32), (2, 2)))
    w_down = centred(key_list[4], (EXPERTS, EXPERT_FF, D), (EXPERT_FF // 4) ** -0.5, 0.4375, ((0, 32), (1, 2)))
    expert_ids_keys = jax.random.split(jax.random.fold_in(part_splits[5], 1), TOKENS // TOK_DEV)
    expert_ids_turns = jax.random.permutation(jax.random.fold_in(part_splits[5], 3), TOKENS // TOK_DEV)
    expert_ids = jax.vmap(lambda own, number: deal_out(jax.random.fold_in(part_splits[5], 2), own, number, TOK_DEV, EXPERTS, TOPK, CAP, 2))(expert_ids_keys, expert_ids_turns).reshape((TOKENS, TOPK))
    route_weights = jnp.clip(jnp.exp(math.log(1.0) - 2.9957323 * jax.random.uniform(part_splits[6], (TOKENS, TOPK), jnp.float32) ** level_of(part_splits[6], (TOKENS, TOPK), ((0, 64),), -0.2, 0.2)), 0.05, 1.0)
    return {"tokens": tokens, "norm_gain": norm_gain, "w_gate": w_gate, "w_up": w_up, "w_down": w_down, "expert_ids": expert_ids, "route_weights": route_weights}


epsilon = 1e-06

def reference(tokens, norm_gain, w_gate, w_up, w_down, expert_ids, route_weights):
    stream = tokens.astype(jnp.float32)
    normed = (stream * lax.rsqrt(lax.optimization_barrier(jnp.mean(stream * stream, axis=-1, keepdims=True)) + epsilon) * norm_gain).astype(jnp.bfloat16)
    route = route_weights / lax.optimization_barrier(jnp.sum(route_weights, axis=-1, keepdims=True))
    flat_ids = expert_ids.reshape(-1).astype(jnp.int32)
    flat_route = route.reshape(-1)
    row_total = flat_ids.shape[0]
    row_bound = CAP * N_EXPERT * N_TENSOR
    half_units = EXPERT_FF // N_TENSOR
    position = jnp.arange(row_total, dtype=jnp.int32)

    def per_expert(running, expert):
        sort_key = jnp.where(flat_ids == expert, position, position + row_total)
        chosen = jnp.argsort(sort_key)[:row_bound].astype(jnp.int32)
        is_valid = flat_ids[chosen] == expert
        owner_row = (chosen // TOPK).astype(jnp.int32)
        rows_in = normed[owner_row]
        gate_cols = w_gate[expert]
        up_cols = w_up[expert]
        down_rows = w_down[expert]
        expert_sum = jnp.zeros((row_bound, D), jnp.float32)
        for core_index in range(N_TENSOR):
            low = core_index * half_units
            gate_pre = jnp.dot(rows_in, gate_cols[:, low:low + half_units], preferred_element_type=jnp.float32)
            up_pre = jnp.dot(rows_in, up_cols[:, low:low + half_units], preferred_element_type=jnp.float32)
            hidden = (jax.nn.silu(gate_pre) * up_pre).astype(jnp.bfloat16)
            partial_value = jnp.dot(hidden, down_rows[low:low + half_units, :], preferred_element_type=jnp.float32)
            rounded = lax.optimization_barrier(partial_value.astype(jnp.bfloat16))
            expert_sum = expert_sum + rounded.astype(jnp.float32)
        expert_out = lax.optimization_barrier(expert_sum.astype(jnp.bfloat16)).astype(jnp.float32)
        row_weight = jnp.where(is_valid, flat_route[chosen], jnp.float32(0.0))
        running = running.at[owner_row].add(row_weight[:, None] * expert_out)
        return (running, None)
    running, _ = lax.scan(per_expert, jnp.zeros((TOKENS, D), jnp.float32), jnp.arange(EXPERTS, dtype=jnp.int32))
    return running.astype(jnp.bfloat16)
```

```python
import jax
import jax.numpy as jnp
from jax import lax
from jax.sharding import PartitionSpec as P

epsilon = 1e-06
LANES = 128


def route_lanes(expert_ids, route, experts):
    chosen = expert_ids[:, :, None] == jnp.arange(experts, dtype=jnp.int32)[None, None, :]
    dense = jnp.sum(jnp.where(chosen, route[:, :, None], 0.0), axis=1)
    high = lax.reduce_precision(dense, 8, 7)
    low = dense - high
    width = -(-2 * experts // LANES) * LANES
    table = jnp.concatenate([high, low], axis=1)
    return jnp.pad(table, ((0, 0), (0, width - 2 * experts))).astype(jnp.bfloat16)


def shards(tokens, norm_gain, w_gate, w_up, w_down, expert_ids, route_weights):
    features = tokens.shape[1]
    experts = lax.axis_size("expert")
    cores = lax.axis_size("tensor")
    half = experts // 2
    me = lax.axis_index("expert")

    def ring(step):
        pairs = []
        for place in range(experts):
            pairs.append((place * cores, (place + step) % experts * cores))
            pairs.append((place * cores + 1, (place - step) % experts * cores + 1))
        return pairs

    out_ring, back_ring = ring(1), ring(-1)
    swap = [(0, 1), (1, 0)]

    stream = tokens.astype(jnp.float32)
    normed = (
        stream * lax.rsqrt(jnp.mean(stream * stream, axis=-1, keepdims=True) + epsilon) * norm_gain
    ).astype(jnp.bfloat16)
    route = route_weights / jnp.sum(route_weights, axis=-1, keepdims=True)
    block = jnp.concatenate([normed, route_lanes(expert_ids, route, experts)], axis=1)

    own = [block]
    other = [lax.ppermute(block, "tensor", swap)]
    weights = [(w_gate[0], w_up[0], w_down[0])]
    weights.append(tuple(lax.ppermute(w, "tensor", swap) for w in weights[0]))

    for step in range(1, half + 1):
        own.append(lax.ppermute(own[-1], ("expert", "tensor"), out_ring))
        if step < half:
            other.append(lax.ppermute(other[-1], ("expert", "tensor"), out_ring))

    def expert_block(parts):
        rows = jnp.concatenate(parts, axis=0)
        inputs = rows[:, :features]
        table = rows[:, features:].astype(jnp.float32)
        here = lax.broadcasted_iota(jnp.int32, table.shape, 1)
        weight = jnp.sum(
            jnp.where((here == me) | (here == me + experts), table, 0.0), axis=1, keepdims=True
        )
        total = None
        for gate, up, down in weights:
            gate_pre = jnp.dot(inputs, gate, preferred_element_type=jnp.float32)
            up_pre = jnp.dot(inputs, up, preferred_element_type=jnp.float32)
            hidden = (jax.nn.silu(gate_pre) * up_pre).astype(jnp.bfloat16)
            part = jnp.dot(hidden, down, preferred_element_type=jnp.float32)
            total = part if total is None else total + part
        value = (total * weight).astype(jnp.bfloat16)
        count = parts[0].shape[0]
        return [value[i * count : (i + 1) * count] for i in range(len(parts))]

    own_out, other_out = {}, {}
    steps = [[0, 1]] + [[s, s + 1] for s in range(2, half, 2)] + [[half]]
    for group in steps:
        keys = [(own_out, s, own[s]) for s in group]
        keys += [(other_out, s, other[s]) for s in group if 0 < s < half]
        for (store, s, _), value in zip(keys, expert_block([k[2] for k in keys])):
            store[s] = value

    def add(a, b):
        return (a.astype(jnp.float32) + b.astype(jnp.float32)).astype(jnp.bfloat16)

    own_sum, other_sum = own_out[half], other_out[half - 1]
    for step in range(half, 0, -1):
        own_sum = lax.ppermute(own_sum, ("expert", "tensor"), back_ring)
        if step > 1:
            own_sum = add(own_sum, own_out[step - 1])
        if step < half:
            other_sum = lax.ppermute(other_sum, ("expert", "tensor"), back_ring)
            if step > 1:
                other_sum = add(other_sum, other_out[step - 1])
    passed = lax.ppermute(other_sum, "tensor", swap)
    mixed = own_sum.astype(jnp.float32) + passed.astype(jnp.float32) + own_out[0].astype(jnp.float32)
    return mixed.astype(jnp.bfloat16)


def solution(mesh):
    in_specs = (
        P(("group", "expert", "tensor"), None),
        P(),
        P("expert", None, "tensor"),
        P("expert", None, "tensor"),
        P("expert", "tensor", None),
        P(("group", "expert", "tensor"), None),
        P(("group", "expert", "tensor"), None),
    )
    out_specs = P(("group", "expert", "tensor"), None)
    return jax.shard_map(shards, mesh=mesh, in_specs=in_specs, out_specs=out_specs, check_vma=False)
```

```python
import functools

import jax
import jax.numpy as jnp
from jax import lax
from jax.experimental import pallas as pl
from jax.experimental.pallas import tpu as pltpu
from jax.sharding import PartitionSpec as P


epsilon = 1e-06
LANES = 128
CHUNKS = 2
K_BLOCK = 1024
N_BLOCK = 1024


def route_lanes(expert_ids, route, experts):
    chosen = expert_ids[:, :, None] == jnp.arange(experts, dtype=jnp.int32)[None, None, :]
    dense = jnp.sum(jnp.where(chosen, route[:, :, None], 0.0), axis=1)
    high = lax.reduce_precision(dense, 8, 7)
    low = dense - high
    width = -(-2 * experts // LANES) * LANES
    table = jnp.concatenate([high, low], axis=1)
    return jnp.pad(table, ((0, 0), (0, width - 2 * experts))).astype(jnp.bfloat16)


def product(chunks, columns, own_ref, other_ref, total):
    rows = jnp.concatenate([c[:, columns] for c in chunks], axis=0)
    weights = jnp.concatenate([own_ref[...], other_ref[...]], axis=1)
    total[...] += jnp.dot(rows, weights, preferred_element_type=jnp.float32)


def gate_kernel(count, features, experts, me_ref, *refs):
    chunks = refs[:count]
    own_ref, other_ref, gate_ref, weight_ref = refs[count:]
    step = pl.program_id(0)
    block = own_ref.shape[0]

    @pl.when(step == 0)
    def _():
        gate_ref[...] = jnp.zeros_like(gate_ref)
        table = jnp.concatenate([c[:, features:] for c in chunks], axis=0).astype(jnp.float32)
        lane = lax.broadcasted_iota(jnp.int32, table.shape, 1)
        here = (lane == me_ref[0]) | (lane == me_ref[0] + experts)
        weight = jnp.sum(jnp.where(here, table, 0.0), axis=1, keepdims=True)
        weight_ref[...] = jnp.broadcast_to(weight, weight_ref.shape)

    columns = pl.ds(pl.multiple_of(step * block, block), block)
    product(chunks, columns, own_ref, other_ref, gate_ref)


def up_kernel(count, gate_ref, *refs):
    chunks = refs[:count]
    own_ref, other_ref, hidden_ref, total = refs[count:]
    step = pl.program_id(0)
    block = own_ref.shape[0]

    @pl.when(step == 0)
    def _():
        total[...] = jnp.zeros_like(total)

    columns = pl.ds(pl.multiple_of(step * block, block), block)
    product(chunks, columns, own_ref, other_ref, total)

    @pl.when(step == pl.num_programs(0) - 1)
    def _():
        value = gate_ref[...]
        hidden_ref[...] = (value / (1.0 + jnp.exp(-value)) * total[...]).astype(hidden_ref.dtype)


def down_kernel(hidden_ref, weight_ref, own_ref, other_ref, *out_refs):
    down = jnp.concatenate([own_ref[...], other_ref[...]], axis=0)
    total = jnp.dot(hidden_ref[...], down, preferred_element_type=jnp.float32)
    total = (total * weight_ref[:, :1]).astype(out_refs[0].dtype)
    rows = out_refs[0].shape[0]
    for n, out_ref in enumerate(out_refs):
        out_ref[...] = total[n * rows : (n + 1) * rows]


def expert_rows(chunks, me, own, other, experts, features):
    count, height = len(chunks), chunks[0].shape[0]
    rows = count * height
    units = own[0].shape[1]
    whole = pl.BlockSpec(memory_space=pltpu.VMEM)
    block = min(K_BLOCK, features)
    weight_spec = pl.BlockSpec((block, units), lambda k: (k, 0))
    cost = pl.CostEstimate(
        flops=4 * rows * features * units,
        bytes_accessed=4 * features * units + 2 * rows * features,
        transcendentals=0,
    )
    params = pltpu.CompilerParams(vmem_limit_bytes=20 * 2**20)
    gate, weight = pl.pallas_call(
        functools.partial(gate_kernel, count, features, experts),
        grid=(features // block,),
        in_specs=[pl.BlockSpec(memory_space=pltpu.SMEM)] + [whole] * count + [weight_spec] * 2,
        out_specs=[
            pl.BlockSpec((rows, 2 * units), lambda k: (0, 0)),
            pl.BlockSpec((rows, LANES), lambda k: (0, 0)),
        ],
        out_shape=[
            jax.ShapeDtypeStruct((rows, 2 * units), jnp.float32),
            jax.ShapeDtypeStruct((rows, LANES), jnp.float32),
        ],
        cost_estimate=cost,
        compiler_params=params,
        name="gate",
    )(me, *chunks, own[0], other[0])
    hidden = pl.pallas_call(
        functools.partial(up_kernel, count),
        grid=(features // block,),
        in_specs=[whole] + [whole] * count + [weight_spec] * 2,
        out_specs=pl.BlockSpec((rows, 2 * units), lambda k: (0, 0)),
        out_shape=jax.ShapeDtypeStruct((rows, 2 * units), jnp.bfloat16),
        scratch_shapes=[pltpu.VMEM((rows, 2 * units), jnp.float32)],
        cost_estimate=cost,
        compiler_params=params,
        name="up",
    )(gate, *chunks, own[1], other[1])
    width = min(N_BLOCK, features)
    down_spec = pl.BlockSpec((units, width), lambda n: (0, n))
    return pl.pallas_call(
        down_kernel,
        grid=(features // width,),
        in_specs=[whole, whole, down_spec, down_spec],
        out_specs=[pl.BlockSpec((height, width), lambda n: (0, n))] * count,
        out_shape=[jax.ShapeDtypeStruct((height, features), jnp.bfloat16)] * count,
        cost_estimate=cost,
        compiler_params=pltpu.CompilerParams(vmem_limit_bytes=16 * 2**20),
        name="down",
    )(hidden, weight, own[2], other[2])


def return_order(half):
    order = list(range(CHUNKS, 2 * CHUNKS)) + list(range(CHUNKS))
    return [(s, i) for s in range(half, 0, -1) for i in order if s < half or i < CHUNKS]


def shards(tokens, norm_gain, w_gate, w_up, w_down, expert_ids, route_weights):
    row_count, features = tokens.shape
    experts = lax.axis_size("expert")
    cores = lax.axis_size("tensor")
    half = experts // 2
    me = lax.axis_index("expert").astype(jnp.int32).reshape(1)
    rows = row_count // CHUNKS

    def ring(step):
        pairs = []
        for place in range(experts):
            pairs.append((place * cores, (place + step) % experts * cores))
            pairs.append((place * cores + 1, (place - step) % experts * cores + 1))
        return pairs

    out_ring, back_ring = ring(1), ring(-1)
    swap = [(0, 1), (1, 0)]

    stream = tokens.astype(jnp.float32)
    normed = (
        stream * lax.rsqrt(jnp.mean(stream * stream, axis=-1, keepdims=True) + epsilon) * norm_gain
    ).astype(jnp.bfloat16)
    route = route_weights / jnp.sum(route_weights, axis=-1, keepdims=True)
    block = jnp.concatenate([normed, route_lanes(expert_ids, route, experts)], axis=1)
    block, me = lax.optimization_barrier((block, me))

    mine = [block[i * rows : (i + 1) * rows] for i in range(CHUNKS)]
    chunk = [mine + [lax.ppermute(c, "tensor", swap) for c in mine]]
    own = (w_gate[0], w_up[0], w_down[0])
    other = tuple(lax.ppermute(w, "tensor", swap) for w in own)
    for step in range(1, half + 1):
        kept = 2 * CHUNKS if step < half else CHUNKS
        moved = []
        for i in range(kept):
            moved.append(lax.ppermute(chunk[-1][i], ("expert", "tensor"), out_ring))
        chunk.append(moved)

    places = [(s, i) for s in range(1, half + 1) for i in range(len(chunk[s]))]
    places += [(0, i) for i in range(CHUNKS)]
    group_size = 8 * CHUNKS
    out = {}
    for first in range(0, len(places), group_size):
        group = places[first : first + group_size]
        parts = [chunk[s][i] for s, i in group]
        out.update(zip(group, expert_rows(parts, me, own, other, experts, features)))

    def add(a, b):
        return (a.astype(jnp.float32) + b.astype(jnp.float32)).astype(jnp.bfloat16)

    total = {i: out[(half if i < CHUNKS else half - 1, i)] for i in range(2 * CHUNKS)}
    last = None
    for step, i in return_order(half):
        arrived = lax.ppermute(total[i], ("expert", "tensor"), back_ring)
        if last is not None:
            arrived, total[last] = lax.optimization_barrier((arrived, total[last]))
        total[i] = add(arrived, out[(step - 1, i)]) if step > 1 else arrived
        last = i
    passed = [lax.ppermute(total[CHUNKS + i], "tensor", swap) for i in range(CHUNKS)]
    mixed = [
        total[i].astype(jnp.float32) + passed[i].astype(jnp.float32) + out[(0, i)].astype(jnp.float32)
        for i in range(CHUNKS)
    ]
    return jnp.concatenate(mixed, axis=0).astype(jnp.bfloat16)


def solution(mesh):
    in_specs = (
        P(("group", "expert", "tensor"), None),
        P(),
        P("expert", None, "tensor"),
        P("expert", None, "tensor"),
        P("expert", "tensor", None),
        P(("group", "expert", "tensor"), None),
        P(("group", "expert", "tensor"), None),
    )
    out_specs = P(("group", "expert", "tensor"), None)

    return jax.shard_map(shards, mesh=mesh, in_specs=in_specs, out_specs=out_specs, check_vma=False)
```

```python
import functools

import jax
import jax.numpy as jnp
from jax import lax
from jax.experimental import pallas as pl
from jax.experimental.pallas import tpu as pltpu
from jax.sharding import PartitionSpec as P


epsilon = 1e-06
LANES = 128
ROW_BLOCK = 256
CHUNKS = 2
K_BLOCK = 1024
N_BLOCK = 1024


def route_lanes(expert_ids, route, experts):
    chosen = expert_ids[:, :, None] == jnp.arange(experts, dtype=jnp.int32)[None, None, :]
    dense = jnp.sum(jnp.where(chosen, route[:, :, None], 0.0), axis=1)
    high = lax.reduce_precision(dense, 8, 7)
    low = dense - high
    width = -(-2 * experts // LANES) * LANES
    table = jnp.concatenate([high, low], axis=1)
    return jnp.pad(table, ((0, 0), (0, width - 2 * experts))).astype(jnp.bfloat16)


def product(chunks, columns, own_ref, other_ref, total):
    height = chunks[0].shape[0]
    weights = jnp.concatenate([own_ref[...], other_ref[...]], axis=1)
    each = max(1, ROW_BLOCK // height)
    for first in range(0, len(chunks), each):
        some = chunks[first : first + each]
        rows = jnp.concatenate([c[:, columns] for c in some], axis=0)
        place = slice(first * height, (first + len(some)) * height)
        total[place, :] += jnp.dot(rows, weights, preferred_element_type=jnp.float32)


def gate_kernel(count, features, experts, me_ref, *refs):
    chunks = refs[:count]
    own_ref, other_ref, gate_ref, weight_ref = refs[count:]
    step = pl.program_id(0)
    block = own_ref.shape[0]

    @pl.when(step == 0)
    def _():
        gate_ref[...] = jnp.zeros_like(gate_ref)
        table = jnp.concatenate([c[:, features:] for c in chunks], axis=0).astype(jnp.float32)
        lane = lax.broadcasted_iota(jnp.int32, table.shape, 1)
        here = (lane == me_ref[0]) | (lane == me_ref[0] + experts)
        weight = jnp.sum(jnp.where(here, table, 0.0), axis=1, keepdims=True)
        weight_ref[...] = jnp.broadcast_to(weight, weight_ref.shape)

    columns = pl.ds(pl.multiple_of(step * block, block), block)
    product(chunks, columns, own_ref, other_ref, gate_ref)


def up_kernel(count, gate_ref, *refs):
    chunks = refs[:count]
    own_ref, other_ref, hidden_ref, total = refs[count:]
    step = pl.program_id(0)
    block = own_ref.shape[0]

    @pl.when(step == 0)
    def _():
        total[...] = jnp.zeros_like(total)

    columns = pl.ds(pl.multiple_of(step * block, block), block)
    product(chunks, columns, own_ref, other_ref, total)

    @pl.when(step == pl.num_programs(0) - 1)
    def _():
        value = gate_ref[...]
        hidden_ref[...] = (value / (1.0 + jnp.exp(-value)) * total[...]).astype(hidden_ref.dtype)


def down_kernel(hidden_ref, weight_ref, own_ref, other_ref, out_ref):
    down = jnp.concatenate([own_ref[...], other_ref[...]], axis=0)
    for first in range(0, out_ref.shape[0], ROW_BLOCK):
        place = slice(first, min(first + ROW_BLOCK, out_ref.shape[0]))
        total = jnp.dot(hidden_ref[place, :], down, preferred_element_type=jnp.float32)
        out_ref[place, :] = (total * weight_ref[place, :1]).astype(out_ref.dtype)


def expert_rows(chunks, me, own, other, experts, features):
    count, height = len(chunks), chunks[0].shape[0]
    rows = count * height
    units = own[0].shape[1]
    whole = pl.BlockSpec(memory_space=pltpu.VMEM)
    block = min(K_BLOCK, features)
    weight_spec = pl.BlockSpec((block, units), lambda k: (k, 0))
    cost = pl.CostEstimate(
        flops=4 * rows * features * units,
        bytes_accessed=4 * features * units + 2 * rows * features,
        transcendentals=0,
    )
    params = pltpu.CompilerParams(vmem_limit_bytes=40 * 2**20)
    gate, weight = pl.pallas_call(
        functools.partial(gate_kernel, count, features, experts),
        grid=(features // block,),
        in_specs=[pl.BlockSpec(memory_space=pltpu.SMEM)] + [whole] * count + [weight_spec] * 2,
        out_specs=[
            pl.BlockSpec((rows, 2 * units), lambda k: (0, 0)),
            pl.BlockSpec((rows, LANES), lambda k: (0, 0)),
        ],
        out_shape=[
            jax.ShapeDtypeStruct((rows, 2 * units), jnp.float32),
            jax.ShapeDtypeStruct((rows, LANES), jnp.float32),
        ],
        cost_estimate=cost,
        compiler_params=params,
        name="gate",
    )(me, *chunks, own[0], other[0])
    hidden = pl.pallas_call(
        functools.partial(up_kernel, count),
        grid=(features // block,),
        in_specs=[whole] + [whole] * count + [weight_spec] * 2,
        out_specs=pl.BlockSpec((rows, 2 * units), lambda k: (0, 0)),
        out_shape=jax.ShapeDtypeStruct((rows, 2 * units), jnp.bfloat16),
        scratch_shapes=[pltpu.VMEM((rows, 2 * units), jnp.float32)],
        cost_estimate=cost,
        compiler_params=params,
        name="up",
    )(gate, *chunks, own[1], other[1])
    width = min(N_BLOCK, features)
    down_spec = pl.BlockSpec((units, width), lambda n: (0, n))
    return pl.pallas_call(
        down_kernel,
        grid=(features // width,),
        in_specs=[whole, whole, down_spec, down_spec],
        out_specs=pl.BlockSpec((rows, width), lambda n: (0, n)),
        out_shape=jax.ShapeDtypeStruct((rows, features), jnp.bfloat16),
        cost_estimate=cost,
        compiler_params=pltpu.CompilerParams(vmem_limit_bytes=32 * 2**20),
        name="down",
    )(hidden, weight, own[2], other[2])


def return_order(half):
    order = list(range(CHUNKS, 2 * CHUNKS)) + list(range(CHUNKS))
    return [(s, i) for s in range(half, 0, -1) for i in order if s < half or i < CHUNKS]


def shards(tokens, norm_gain, w_gate, w_up, w_down, expert_ids, route_weights):
    row_count, features = tokens.shape
    experts = lax.axis_size("expert")
    cores = lax.axis_size("tensor")
    half = experts // 2
    me = lax.axis_index("expert").astype(jnp.int32).reshape(1)
    rows = row_count // CHUNKS

    def ring(step):
        pairs = []
        for place in range(experts):
            pairs.append((place * cores, (place + step) % experts * cores))
            pairs.append((place * cores + 1, (place - step) % experts * cores + 1))
        return pairs

    out_ring, back_ring = ring(1), ring(-1)
    swap = [(0, 1), (1, 0)]

    stream = tokens.astype(jnp.float32)
    normed = (
        stream * lax.rsqrt(jnp.mean(stream * stream, axis=-1, keepdims=True) + epsilon) * norm_gain
    ).astype(jnp.bfloat16)
    route = route_weights / jnp.sum(route_weights, axis=-1, keepdims=True)
    block = jnp.concatenate([normed, route_lanes(expert_ids, route, experts)], axis=1)
    block, me = lax.optimization_barrier((block, me))

    mine = [block[i * rows : (i + 1) * rows] for i in range(CHUNKS)]
    chunk = [mine + [lax.ppermute(c, "tensor", swap) for c in mine]]
    own = (w_gate[0], w_up[0], w_down[0])
    other = tuple(lax.ppermute(w, "tensor", swap) for w in own)
    for step in range(1, half + 1):
        kept = 2 * CHUNKS if step < half else CHUNKS
        moved = []
        for i in range(kept):
            moved.append(lax.ppermute(chunk[-1][i], ("expert", "tensor"), out_ring))
        chunk.append(moved)

    places = [(s, i) for s in range(1, half + 1) for i in range(len(chunk[s]))]
    places += [(0, i) for i in range(CHUNKS)]
    value = expert_rows([chunk[s][i] for s, i in places], me, own, other, experts, features)

    def out(step, i):
        first = places.index((step, i)) * rows
        return value[first : first + rows]

    total = {i: out(half if i < CHUNKS else half - 1, i) for i in range(2 * CHUNKS)}
    last = None
    for step, i in return_order(half):
        arrived = lax.ppermute(total[i], ("expert", "tensor"), back_ring)
        if last is not None:
            arrived, _ = lax.optimization_barrier((arrived, total[last]))
        if step > 1:
            here = out(step - 1, i).astype(jnp.float32)
            total[i] = (arrived.astype(jnp.float32) + here).astype(jnp.bfloat16)
        else:
            total[i] = arrived
        last = i
    passed = [lax.ppermute(total[CHUNKS + i], "tensor", swap) for i in range(CHUNKS)]
    mixed = [
        total[i].astype(jnp.float32) + passed[i].astype(jnp.float32) + out(0, i).astype(jnp.float32)
        for i in range(CHUNKS)
    ]
    return jnp.concatenate(mixed, axis=0).astype(jnp.bfloat16)


def solution(mesh):
    in_specs = (
        P(("group", "expert", "tensor"), None),
        P(),
        P("expert", None, "tensor"),
        P("expert", None, "tensor"),
        P("expert", "tensor", None),
        P(("group", "expert", "tensor"), None),
        P(("group", "expert", "tensor"), None),
    )
    out_specs = P(("group", "expert", "tensor"), None)

    return jax.shard_map(shards, mesh=mesh, in_specs=in_specs, out_specs=out_specs, check_vma=False)
```

```python
import functools

import jax
import jax.numpy as jnp
from jax import lax
from jax.experimental import pallas as pl
from jax.experimental.pallas import tpu as pltpu
from jax.sharding import PartitionSpec as P


epsilon = 1e-06
LANES = 128
ROW_BLOCK = 256
CHUNKS = 2
CUTS = 3
K_BLOCK = 1024
N_BLOCK = 1024


def route_lanes(expert_ids, route, experts):
    chosen = expert_ids[:, :, None] == jnp.arange(experts, dtype=jnp.int32)[None, None, :]
    dense = jnp.sum(jnp.where(chosen, route[:, :, None], 0.0), axis=1)
    high = lax.reduce_precision(dense, 8, 7)
    low = dense - high
    width = -(-2 * experts // LANES) * LANES
    table = jnp.concatenate([high, low], axis=1)
    return jnp.pad(table, ((0, 0), (0, width - 2 * experts))).astype(jnp.bfloat16)


def product(chunks, columns, own_ref, other_ref, total):
    height = chunks[0].shape[0]
    weights = jnp.concatenate([own_ref[...], other_ref[...]], axis=1)
    each = max(1, ROW_BLOCK // height)
    for first in range(0, len(chunks), each):
        some = chunks[first : first + each]
        rows = jnp.concatenate([c[:, columns] for c in some], axis=0)
        place = slice(first * height, (first + len(some)) * height)
        total[place, :] += jnp.dot(rows, weights, preferred_element_type=jnp.float32)


def gate_kernel(count, features, experts, me_ref, *refs):
    chunks = refs[:count]
    own_ref, other_ref, gate_ref, weight_ref = refs[count:]
    step = pl.program_id(0)
    block = own_ref.shape[0]

    @pl.when(step == 0)
    def _():
        gate_ref[...] = jnp.zeros_like(gate_ref)
        table = jnp.concatenate([c[:, features:] for c in chunks], axis=0).astype(jnp.float32)
        lane = lax.broadcasted_iota(jnp.int32, table.shape, 1)
        here = (lane == me_ref[0]) | (lane == me_ref[0] + experts)
        weight = jnp.sum(jnp.where(here, table, 0.0), axis=1, keepdims=True)
        weight_ref[...] = jnp.broadcast_to(weight, weight_ref.shape)

    columns = pl.ds(pl.multiple_of(step * block, block), block)
    product(chunks, columns, own_ref, other_ref, gate_ref)


def up_kernel(count, gate_ref, *refs):
    chunks = refs[:count]
    own_ref, other_ref, hidden_ref, total = refs[count:]
    step = pl.program_id(0)
    block = own_ref.shape[0]

    @pl.when(step == 0)
    def _():
        total[...] = jnp.zeros_like(total)

    columns = pl.ds(pl.multiple_of(step * block, block), block)
    product(chunks, columns, own_ref, other_ref, total)

    @pl.when(step == pl.num_programs(0) - 1)
    def _():
        value = gate_ref[...]
        hidden_ref[...] = (value / (1.0 + jnp.exp(-value)) * total[...]).astype(hidden_ref.dtype)


def down_kernel(hidden_ref, weight_ref, own_ref, other_ref, out_ref):
    down = jnp.concatenate([own_ref[...], other_ref[...]], axis=0)
    for first in range(0, out_ref.shape[0], ROW_BLOCK):
        place = slice(first, min(first + ROW_BLOCK, out_ref.shape[0]))
        total = jnp.dot(hidden_ref[place, :], down, preferred_element_type=jnp.float32)
        out_ref[place, :] = (total * weight_ref[place, :1]).astype(out_ref.dtype)


def expert_rows(chunks, me, own, other, experts, features):
    count, height = len(chunks), chunks[0].shape[0]
    rows = count * height
    units = own[0].shape[1]
    whole = pl.BlockSpec(memory_space=pltpu.VMEM)
    block = min(K_BLOCK, features)
    weight_spec = pl.BlockSpec((block, units), lambda k: (k, 0))
    cost = pl.CostEstimate(
        flops=4 * rows * features * units,
        bytes_accessed=4 * features * units + 2 * rows * features,
        transcendentals=0,
    )
    params = pltpu.CompilerParams(vmem_limit_bytes=40 * 2**20)
    gate, weight = pl.pallas_call(
        functools.partial(gate_kernel, count, features, experts),
        grid=(features // block,),
        in_specs=[pl.BlockSpec(memory_space=pltpu.SMEM)] + [whole] * count + [weight_spec] * 2,
        out_specs=[
            pl.BlockSpec((rows, 2 * units), lambda k: (0, 0)),
            pl.BlockSpec((rows, LANES), lambda k: (0, 0)),
        ],
        out_shape=[
            jax.ShapeDtypeStruct((rows, 2 * units), jnp.float32),
            jax.ShapeDtypeStruct((rows, LANES), jnp.float32),
        ],
        cost_estimate=cost,
        compiler_params=params,
        name="gate",
    )(me, *chunks, own[0], other[0])
    hidden = pl.pallas_call(
        functools.partial(up_kernel, count),
        grid=(features // block,),
        in_specs=[whole] + [whole] * count + [weight_spec] * 2,
        out_specs=pl.BlockSpec((rows, 2 * units), lambda k: (0, 0)),
        out_shape=jax.ShapeDtypeStruct((rows, 2 * units), jnp.bfloat16),
        scratch_shapes=[pltpu.VMEM((rows, 2 * units), jnp.float32)],
        cost_estimate=cost,
        compiler_params=params,
        name="up",
    )(gate, *chunks, own[1], other[1])
    width = min(N_BLOCK, features)
    down_spec = pl.BlockSpec((units, width), lambda n: (0, n))
    return pl.pallas_call(
        down_kernel,
        grid=(features // width,),
        in_specs=[whole, whole, down_spec, down_spec],
        out_specs=pl.BlockSpec((rows, width), lambda n: (0, n)),
        out_shape=jax.ShapeDtypeStruct((rows, features), jnp.bfloat16),
        cost_estimate=cost,
        compiler_params=pltpu.CompilerParams(vmem_limit_bytes=32 * 2**20),
        name="down",
    )(hidden, weight, own[2], other[2])


def return_order(half):
    order = list(range(CUTS, 2 * CUTS)) + list(range(CUTS))
    return [(s, i) for s in range(half, 0, -1) for i in order if s < half or i < CUTS]


def shards(tokens, norm_gain, w_gate, w_up, w_down, expert_ids, route_weights):
    row_count, features = tokens.shape
    experts = lax.axis_size("expert")
    cores = lax.axis_size("tensor")
    half = experts // 2
    me = lax.axis_index("expert").astype(jnp.int32).reshape(1)
    rows = row_count // CHUNKS

    def ring(step):
        pairs = []
        for place in range(experts):
            pairs.append((place * cores, (place + step) % experts * cores))
            pairs.append((place * cores + 1, (place - step) % experts * cores + 1))
        return pairs

    out_ring, back_ring = ring(1), ring(-1)
    swap = [(0, 1), (1, 0)]

    stream = tokens.astype(jnp.float32)
    scale = lax.rsqrt(jnp.mean(stream * stream, axis=-1, keepdims=True) + epsilon)
    normed = (stream * scale * norm_gain).astype(jnp.bfloat16)
    route = route_weights / jnp.sum(route_weights, axis=-1, keepdims=True)
    block = jnp.concatenate([normed, route_lanes(expert_ids, route, experts)], axis=1)
    block, me = lax.optimization_barrier((block, me))

    mine = [block[i * rows : (i + 1) * rows] for i in range(CHUNKS)]
    chunk = [mine + [lax.ppermute(c, "tensor", swap) for c in mine]]
    own = (w_gate[0], w_up[0], w_down[0])
    other = []
    for weight in own:
        other.append(lax.ppermute(weight, "tensor", swap))
    for step in range(1, half + 1):
        kept = 2 * CHUNKS if step < half else CHUNKS
        moved = []
        for i in range(kept):
            moved.append(lax.ppermute(chunk[-1][i], ("expert", "tensor"), out_ring))
        chunk.append(moved)

    places = [(s, i) for s in range(1, half + 1) for i in range(len(chunk[s]))]
    places += [(0, i) for i in range(CHUNKS)]
    value = expert_rows([chunk[s][i] for s, i in places], me, own, other, experts, features)

    wide = -(-features // (CUTS * LANES)) * LANES

    def out(step, i):
        first = places.index((step, i // CUTS * CHUNKS)) * rows
        cut = i % CUTS * wide
        return value[first : first + row_count, cut : min(cut + wide, features)]

    total = {i: out(half if i < CUTS else half - 1, i) for i in range(2 * CUTS)}
    last = None
    for step, i in return_order(half):
        arrived = lax.ppermute(total[i], ("expert", "tensor"), back_ring)
        if last is not None:
            arrived, _ = lax.optimization_barrier((arrived, total[last]))
        if step > 1:
            here = out(step - 1, i).astype(jnp.float32)
            total[i] = (arrived.astype(jnp.float32) + here).astype(jnp.bfloat16)
        else:
            total[i] = arrived
        last = i
    passed = [lax.ppermute(total[CUTS + i], "tensor", swap) for i in range(CUTS)]
    mixed = [
        total[i].astype(jnp.float32) + passed[i].astype(jnp.float32) + out(0, i).astype(jnp.float32)
        for i in range(CUTS)
    ]
    return jnp.concatenate(mixed, axis=1).astype(jnp.bfloat16)


def solution(mesh):
    in_specs = (
        P(("group", "expert", "tensor"), None),
        P(),
        P("expert", None, "tensor"),
        P("expert", None, "tensor"),
        P("expert", "tensor", None),
        P(("group", "expert", "tensor"), None),
        P(("group", "expert", "tensor"), None),
    )
    out_specs = P(("group", "expert", "tensor"), None)

    return jax.shard_map(shards, mesh=mesh, in_specs=in_specs, out_specs=out_specs, check_vma=False)
```
